32 devices in a mesh: seq: 8 (over z, y), head: 4 (over x, core).
Axes of the slice: x: 2, y: 2, z: 4, core: 2. Of those that a mesh axis runs over, the one named last changes fastest.
Arguments:
- query: bfloat16 [512, 2048], P('seq', 'head'), may hold values from -16 to 16
- key_states: bfloat16 [512, 2048], P('seq', 'head'), may hold values from -16 to 16
- value_states: bfloat16 [512, 2048], P('seq', 'head'), may hold values from -6 to 6
- doc_ids: int32 [512], P('seq'), may hold values from 0 to 3, never falling along the last dimension, each value on 1 to 256 neighbouring positions
- out_weight: bfloat16 [2048, 4096], P('head', 'seq'), may hold values from -0.1875 to 0.1875
- residual: bfloat16 [512, 4096], P('seq', 'head'), may hold values from -6 to 6
Outputs:
- mixed: bfloat16 [512, 4096], P('seq', 'head')
The draws below stay inside these ranges and needn't reach their ends.
Inputs may be any that keep to these rules, and one draw needn't show every extreme that they name: doc_ids never fall along the sequence; every document has 1 to 256 positions, and one has exactly 256.
All inputs are finite; a program needn't handle non-finite values.
Results may differ from the reference program's by a relative error of at most 0.0055.
Values may be sent and summed in bfloat16 or wider, within the bound.
A program may use at most 64 MiB of HBM per device.

```python
import math
import jax
import jax.numpy as jnp
import numpy as np
from jax import lax

D = 4096
HEAD_DIM = 128
HEADS = 16
DOCS = 4
SEQ = 512
DOC_MOST = 256


def drawn_pair(key):
    base = jax.random.fold_in(key, 7)
    first, second = jax.random.split(base, 2)
    width = HEADS * HEAD_DIM
    queries = 1.7 * jnp.clip(jax.random.normal(first, (SEQ, width), jnp.float32), -4.5, 4.5)
    keys = 1.7 * jnp.clip(jax.random.normal(second, (SEQ, width), jnp.float32), -4.5, 4.5)
    return (queries, keys)


def draw_query(key, part):
    return drawn_pair(key)[0].astype(jnp.bfloat16)


def draw_key_states(key, part):
    return drawn_pair(key)[1].astype(jnp.bfloat16)


def spiked(drawn, rng, source, target, blocks, factor):
    owner, partner = [(jnp.arange(drawn.shape[position]) // (drawn.shape[position] // blocks)).reshape([-1 if axis == position else 1 for axis in range(drawn.ndim)]) for position in (source, target)]
    chosen = jax.random.permutation(rng, blocks)[partner]
    strong = (owner == chosen) | (owner == (partner + blocks // 2) % blocks)
    return jnp.where(strong, factor * drawn, drawn)


def block_scale(own_key, dims, cuts, least, largest):
    def one(dim, parts):
        heights = jax.random.uniform(jax.random.fold_in(jax.random.fold_in(own_key, 6), dim), (parts,), jnp.float32, least / len(cuts), largest / len(cuts))
        return jnp.repeat(jnp.exp(heights), dims[dim] // parts).reshape((-1,) + (1,) * (len(dims) - dim - 1))

    level = one(*cuts[0])
    for cut in cuts[1:]:
        level = level * one(*cut)
    return level


def split_up(count, total, most, skew):
    portions = [(1 << 20) // math.isqrt(standing ** skew) + 1 for standing in range(2, count + 1)]
    spare, given = total - most - (count - 1), [1] * (count - 1)
    while spare > 0:
        movable = [i for i in range(count - 1) if given[i] < most]
        pool, left = sum([portions[i] for i in movable]), spare
        for i in movable:
            addition = min(most - given[i], max(1, left * portions[i] // pool), spare)
            given[i] = given[i] + addition
            spare = spare - addition
    return np.array([most] + given)


def ragged(key, count, total, limit, slope):
    if count == 2:
        one = jax.random.randint(key, (), max(1, total - limit), min(limit, total - 1) + 1)
        return jnp.stack([one, total - one])
    sizes = jnp.asarray(split_up(count, total, limit, slope), jnp.int32)
    twos = (count - 1) // 2
    giver, sink = sizes[1:1 + 2 * twos:2], sizes[2:2 + 2 * twos:2]
    room = jnp.minimum(giver - 1, limit - sink)
    moved = jax.random.randint(jax.random.fold_in(key, 1), (twos,), 0, 1 << 20) % (room + 1)
    sizes = sizes.at[1:1 + 2 * twos:2].set(giver - moved).at[2:2 + 2 * twos:2].set(sink + moved)
    return sizes[jax.random.permutation(jax.random.fold_in(key, 2), count)]


def noise(own_key, shape, deviation, limit, shards=(), held_as=jnp.bfloat16):
    drawn = jax.random.normal(own_key, shape, jnp.float32) * deviation
    if len(shards) > 0:
        drawn = block_scale(own_key, shape, shards, -0.22, 0.18) * drawn
    return jnp.clip(drawn, min=-limit, max=limit).astype(held_as)


def heavy_noise(rng, extent, spread, reach, cuts, heavy, kind=jnp.bfloat16):
    result = spread * jax.random.normal(rng, extent, jnp.float32)
    if cuts:
        result = result * block_scale(rng, extent, cuts, -0.22, 0.18)
    return jnp.clip(spiked(result, jax.random.fold_in(rng, 3), *heavy), -reach, reach).astype(kind)


def setup_inputs(seed: int = 0) -> dict:
    splits = jax.random.split(jax.random.key(seed), 7)
    query = draw_query(jax.random.fold_in(splits[6], 71), 0)
    key_states = draw_key_states(jax.random.fold_in(splits[6], 71), 0)
    value_states = noise(splits[2], (SEQ, HEADS * HEAD_DIM), 1.0, 6.0, ((0, 8), (1, 4)))
    doc_ids = jnp.searchsorted(jnp.cumsum(ragged(splits[3], DOCS, SEQ, DOC_MOST, 1)), jnp.arange(SEQ), side="right").astype(jnp.int32)
    out_weight = heavy_noise(splits[4], (HEADS * HEAD_DIM, D), (HEADS * HEAD_DIM) ** -0.5, 0.1875, ((0, 4), (1, 8)), (0, 1, 8, 2.0))
    residual = noise(splits[5], (SEQ, D), 1.0, 6.0, ((0, 8), (1, 4)))
    return {"query": query, "key_states": key_states, "value_states": value_states, "doc_ids": doc_ids, "out_weight": out_weight, "residual": residual}


masked_score = -1.0e30


def reference(query, key_states, value_states, doc_ids, out_weight, residual):
    positions = jnp.arange(SEQ, dtype=jnp.int32)
    allowed = (positions[None, :] <= positions[:, None]) & (doc_ids[None, :] == doc_ids[:, None])
    query_heads = query.reshape(SEQ, HEADS, HEAD_DIM).transpose(1, 0, 2)
    key_heads = key_states.reshape(SEQ, HEADS, HEAD_DIM).transpose(1, 0, 2)
    value_heads = value_states.reshape(SEQ, HEADS, HEAD_DIM).transpose(1, 0, 2)

    def one_head(operands):
        queries, keys, values = operands
        scores = jnp.dot(queries, keys.T, preferred_element_type=jnp.float32) * (HEAD_DIM ** -0.5)
        scores = jnp.where(allowed, scores, masked_score)
        row_max = jnp.max(scores, axis=1, keepdims=True)
        weights = jnp.where(allowed, jnp.exp(scores - row_max), 0.0)
        row_sum = jnp.sum(weights, axis=1, keepdims=True)
        attended = jnp.dot(weights.astype(jnp.bfloat16), values, preferred_element_type=jnp.float32) / row_sum
        return attended.astype(jnp.bfloat16)

    per_head = lax.map(one_head, (query_heads, key_heads, value_heads))
    attended = per_head.transpose(1, 0, 2).reshape(SEQ, HEADS * HEAD_DIM)
    mixed = residual.astype(jnp.float32) + jnp.dot(attended, out_weight, preferred_element_type=jnp.float32)
    return mixed.astype(jnp.bfloat16)
```

```python
import functools

import jax
import jax.numpy as jnp
from jax import lax
from jax.experimental import pallas as pl
from jax.experimental.pallas import tpu as pltpu
from jax.sharding import PartitionSpec as P

HEAD_DIM = 128


masked_score = -1e30


def to_heads(block):
    return block.reshape(block.shape[0], block.shape[1] // HEAD_DIM, HEAD_DIM)


def attend_block(state, queries, query_pos, query_docs, keys, values, key_pos, key_docs):
    run_max, run_sum, run_acc = state
    scores = jnp.einsum(
        "qhd,khd->hqk", queries, keys, preferred_element_type=jnp.float32
    ) * HEAD_DIM ** (-0.5)
    allowed = (key_pos[None, :] <= query_pos[:, None]) & (key_docs[None, :] == query_docs[:, None])
    scores = jnp.where(allowed[None], scores, masked_score)
    new_max = jnp.maximum(run_max, jnp.max(scores, axis=-1))
    weights = jnp.where(allowed[None], jnp.exp(scores - new_max[..., None]), 0.0)
    run_sum = jnp.sum(weights, axis=-1)
    run_acc = jnp.einsum(
        "hqk,khd->hqd", weights.astype(jnp.bfloat16), values, preferred_element_type=jnp.float32
    )
    return (new_max, run_sum, run_acc)


def shards(query, key_states, value_states, doc_ids, out_weight, residual):
    tok_rows = query.shape[0]
    heads = query.shape[1] // HEAD_DIM
    shard_index = lax.axis_index("seq")
    first_pos = shard_index * tok_rows
    groups = [(query, first_pos + jnp.arange(tok_rows, dtype=jnp.int32), doc_ids)]
    prepared = [(to_heads(block), block_pos, block_docs) for block, block_pos, block_docs in groups]
    initial = tuple(
        (
            (
                jnp.full((heads, block_pos.shape[0]), masked_score, jnp.float32),
                jnp.zeros((heads, block_pos.shape[0]), jnp.float32),
                jnp.zeros((heads, block_pos.shape[0], HEAD_DIM), jnp.float32),
            )
            for block, block_pos, block_docs in groups
        )
    )
    first_row = jnp.int32(0)
    keys = lax.all_gather(key_states, "seq", axis=0, tiled=True)
    values = lax.all_gather(value_states, "seq", axis=0, tiled=True)
    key_docs = lax.all_gather(doc_ids, "seq", axis=0, tiled=True)
    key_pos = jnp.arange(keys.shape[0], dtype=jnp.int32)
    key_heads = to_heads(keys)
    value_heads = to_heads(values)
    updated = []
    for member, state in zip(prepared, initial):
        queries, query_pos, query_docs = member

        def advance(inner, queries=queries, query_pos=query_pos, query_docs=query_docs):
            return attend_block(
                inner, queries, query_pos, query_docs, key_heads, value_heads, key_pos, key_docs
            )

        def unchanged(inner):
            return inner

        updated.append(lax.cond(first_row <= jnp.max(query_pos), advance, unchanged, state))
    finals = tuple(updated)
    outputs = []
    for run_max, run_sum, run_acc in finals:
        normed = run_acc / run_sum[..., None]
        outputs.append(
            jnp.transpose(normed, (1, 0, 2))
            .reshape(normed.shape[1], heads * HEAD_DIM)
            .astype(jnp.bfloat16)
        )
    attended = outputs[0]
    mapped = jnp.dot(
        attended,
        lax.all_gather(out_weight, "seq", axis=1, tiled=True),
        preferred_element_type=jnp.float32,
    )
    summed = lax.psum_scatter(mapped, "head", scatter_dimension=1, tiled=True)
    return (residual.astype(jnp.float32) + summed).astype(jnp.bfloat16)


MESH = pl.DeviceIdType.MESH


def attention(queries, keys, values, doc_row, first_row, pos_rows):
    rows, keep = queries.shape[0], keys.shape[0]
    scores = lax.dot_general(
        queries, keys, (((1,), (1,)), ((), ())), preferred_element_type=jnp.float32
    ) * HEAD_DIM ** (-0.5)
    row_pos = lax.broadcasted_iota(jnp.int32, (rows, keep), 0) + first_row
    col_pos = lax.broadcasted_iota(jnp.int32, (rows, keep), 1)
    docs = jnp.broadcast_to(doc_row, (rows, keep))
    query_docs = jnp.sum(jnp.where(row_pos == col_pos, docs, 0), axis=1, keepdims=True)
    allowed = (col_pos <= row_pos) & (docs == query_docs)
    scores = jnp.where(allowed, scores, masked_score)
    row_max = jnp.max(scores, axis=1, keepdims=True)
    weights = jnp.where(allowed, jnp.exp(scores - row_max), 0.0)
    row_sum = jnp.sum(weights, axis=1, keepdims=True)
    product = jnp.dot(weights.astype(jnp.bfloat16), values, preferred_element_type=jnp.float32)
    return (product / row_sum).astype(jnp.bfloat16)


def fused_kernel(
    n, nh, q_ref, k_ref, v_ref, doc_ref, w_ref, res_ref, out_ref,
    qbuf, kbuf, vbuf, docbuf, att, wbuf, sendbuf, parts, resbuf,
    q_send, q_recv, k_send, k_recv, v_send, v_recv, d_send, d_recv,
    a_send, a_recv, f_send, f_recv, p_send, p_recv, w_sems, res_sem,
):
    me = lax.axis_index("seq")
    head = lax.axis_index("head")
    rows = k_ref.shape[0]
    half = n // 2
    mid = half * rows
    plane, side = me // 2, me % 2
    my_half = me // half
    pair, core = head // 2, head % 2
    partner = pair * 2 + (1 - core)
    wrows, wcols = w_ref.shape[0], w_ref.shape[1] // 2

    w_local = pltpu.make_async_copy(
        w_ref.at[:, pl.ds(pl.multiple_of(core * wcols, wcols), wcols)],
        wbuf.at[pl.ds(pl.multiple_of(core * wrows, wrows), wrows), :],
        w_sems.at[0],
    )
    w_local.start()
    res_copy = pltpu.make_async_copy(res_ref, resbuf, res_sem)
    res_copy.start()

    barrier = pltpu.get_barrier_semaphore()
    for ds_ in range(n):
        for dh in range(nh):
            if ds_ == 0 and dh == 0:
                continue
            pl.semaphore_signal(
                barrier, inc=1,
                device_id=(lax.rem(me + ds_, n), lax.rem(head + dh, nh)),
                device_id_type=MESH,
            )
    pl.semaphore_wait(barrier, n * nh - 1)

    def block(ref, source):
        return ref.at[pl.ds(pl.multiple_of(source * rows, rows), rows), :]

    def lanes(ref, index):
        return ref.at[:, pl.ds(pl.multiple_of(index * HEAD_DIM, HEAD_DIM), HEAD_DIM)]

    def send_kv(kind, dst):
        src, dest, ssem, rsem = kind
        return pltpu.make_async_remote_copy(
            src_ref=lanes(src, dst // 2), dst_ref=block(dest, me),
            send_sem=ssem.at[dst], recv_sem=rsem.at[me],
            device_id=(dst, head), device_id_type=MESH,
        )

    def local_kv(kind):
        src, dest, ssem, rsem = kind
        return pltpu.make_async_copy(lanes(src, plane), block(dest, me), rsem.at[me])

    def send_q(dst):
        return pltpu.make_async_remote_copy(
            src_ref=lanes(q_ref, dst // 2), dst_ref=block(qbuf, me % half),
            send_sem=q_send.at[dst], recv_sem=q_recv.at[me % half],
            device_id=(dst, head), device_id_type=MESH,
        )

    def send_doc(dst):
        return pltpu.make_async_remote_copy(
            src_ref=doc_ref, dst_ref=docbuf.at[me],
            send_sem=d_send.at[dst], recv_sem=d_recv.at[me],
            device_id=(dst, head), device_id_type=MESH,
        )

    kinds = ((k_ref, kbuf, k_send, k_recv), (v_ref, vbuf, v_send, v_recv))

    for off in range(1, n):
        dst = lax.rem(me + off, n)

        @pl.when((dst % 2 == 1) | (my_half == 0))
        def _(dst=dst):
            send_kv(kinds[0], dst).start()

        @pl.when(dst % 2 == my_half)
        def _(dst=dst):
            send_q(dst).start()

        send_doc(dst).start()

        @pl.when((dst % 2 == 1) | (my_half == 0))
        def _(dst=dst):
            send_kv(kinds[1], dst).start()

    w_remote = pltpu.make_async_remote_copy(
        src_ref=w_ref.at[:, pl.ds(pl.multiple_of((1 - core) * wcols, wcols), wcols)],
        dst_ref=wbuf.at[pl.ds(pl.multiple_of(core * wrows, wrows), wrows), :],
        send_sem=w_sems.at[1], recv_sem=w_sems.at[2],
        device_id=(me, partner), device_id_type=MESH,
    )
    w_remote.start()

    @pl.when((side == 1) | (my_half == 0))
    def _():
        for kind in kinds:
            local_kv(kind).start()

    @pl.when(side == my_half)
    def _():
        pltpu.make_async_copy(
            lanes(q_ref, plane), block(qbuf, me % half), q_recv.at[me % half]
        ).start()

    pltpu.make_async_copy(doc_ref, docbuf.at[me], d_recv.at[me]).start()

    def arrived(ref, sem):
        pltpu.make_async_copy(ref, ref, sem).wait()

    for source in range(n):
        arrived(docbuf.at[source], d_recv.at[source])
    for source in range(half):
        arrived(qbuf.at[pl.ds(source * rows, rows), :], q_recv.at[source])
        for _, dest, _, rsem in kinds:
            arrived(dest.at[pl.ds(source * rows, rows), :], rsem.at[source])

    mine_rows = pl.ds(pl.multiple_of(side * mid, mid), mid)

    def columns_of(c, index):
        start = (c * half + index) * HEAD_DIM
        return pl.ds(pl.multiple_of(start, HEAD_DIM), HEAD_DIM)

    doc_row = jnp.concatenate([docbuf[source] for source in range(n)], axis=1)

    @pl.when(side == 0)
    def _():
        att[mine_rows, columns_of(core, plane)] = attention(
            qbuf[...], kbuf[:mid, :], vbuf[:mid, :], doc_row[:, :mid], 0, mid
        )

    @pl.when(side == 1)
    def _():
        for source in range(half, n):
            for _, dest, _, rsem in kinds:
                arrived(dest.at[pl.ds(source * rows, rows), :], rsem.at[source])
        att[mine_rows, columns_of(core, plane)] = attention(
            qbuf[...], kbuf[...], vbuf[...], doc_row, mid, mid
        )

    def att_block(c, source):
        return att.at[
            pl.ds(pl.multiple_of((source % 2) * mid, mid), mid), columns_of(c, source // 2)
        ]

    def att_send(dst):
        return pltpu.make_async_remote_copy(
            src_ref=att_block(core, me), dst_ref=att_block(core, me),
            send_sem=a_send.at[dst], recv_sem=a_recv.at[me],
            device_id=(dst, head), device_id_type=MESH,
        )

    def forward(source):
        return pltpu.make_async_remote_copy(
            src_ref=att_block(core, source), dst_ref=att_block(core, source),
            send_sem=f_send.at[source], recv_sem=f_recv.at[source],
            device_id=(me, partner), device_id_type=MESH,
        )

    order = [half, half + 1, half - 1, half + 2, half - 2, half + 3, half - 3]
    for off in order:
        att_send(lax.rem(me + off, n)).start()
    forward(me).start()
    for off in reversed(order):
        source = lax.rem(me + off, n)
        arrived(att_block(core, source), a_recv.at[source])
        forward(source).start()

    w_local.wait()
    w_remote.wait()
    for source in range(n):
        arrived(att_block(1 - core, source), f_recv.at[source])

    for piece in range(2):
        span = slice(piece * mid, (piece + 1) * mid)
        sendbuf[span, :] = jnp.dot(
            att[span, :], wbuf[...], preferred_element_type=jnp.float32
        ).astype(jnp.bfloat16)

        for target in range(piece * half, (piece + 1) * half):
            src = sendbuf.at[pl.ds(target * rows, rows), :]
            slot = pair * 4 + side * 2 + core
            own = (me == target) & (head == plane)

            @pl.when(own)
            def _(src=src, slot=slot):
                pltpu.make_async_copy(src, parts.at[slot], p_recv.at[slot]).start()

            @pl.when(jnp.logical_not(own))
            def _(src=src, slot=slot, target=target):
                pltpu.make_async_remote_copy(
                    src_ref=src, dst_ref=parts.at[slot],
                    send_sem=p_send.at[target], recv_sem=p_recv.at[slot],
                    device_id=(target, plane), device_id_type=MESH,
                ).start()

    res_copy.wait()
    for s in range(2):
        for c in range(2):
            a, b = s * 2 + c, 4 + s * 2 + c
            arrived(parts.at[a], p_recv.at[a])
            arrived(parts.at[b], p_recv.at[b])
            start = (s * 2 + c) * wcols
            cols = slice(start, start + wcols)
            total = parts[a].astype(jnp.float32) + parts[b].astype(jnp.float32)
            out_ref[:, cols] = (resbuf[:, cols].astype(jnp.float32) + total).astype(jnp.bfloat16)

    for off in range(1, n):
        dst = lax.rem(me + off, n)

        @pl.when((dst % 2 == 1) | (my_half == 0))
        def _(dst=dst):
            for kind in kinds:
                send_kv(kind, dst).wait_send()

        @pl.when(dst % 2 == my_half)
        def _(dst=dst):
            send_q(dst).wait_send()

        send_doc(dst).wait_send()
        att_send(dst).wait_send()
    for source in range(n):
        forward(source).wait_send()
    for target in range(n):
        src = sendbuf.at[pl.ds(target * rows, rows), :]

        @pl.when(jnp.logical_not((me == target) & (head == plane)))
        def _(src=src, target=target):
            pltpu.make_async_copy(src, src, p_send.at[target]).wait()


def fused(n, nh, query, key_states, value_states, doc_ids, out_weight, residual):
    rows, width = key_states.shape
    wrows, wcols = out_weight.shape
    seq = n * rows
    dma = pltpu.SemaphoreType.DMA
    vmem = pl.BlockSpec(memory_space=pltpu.VMEM)
    any_ = pl.BlockSpec(memory_space=pl.ANY)
    bf16 = jnp.bfloat16
    return pl.pallas_call(
        functools.partial(fused_kernel, n, nh),
        out_shape=jax.ShapeDtypeStruct(residual.shape, residual.dtype),
        in_specs=[vmem, vmem, vmem, vmem, any_, any_],
        out_specs=vmem,
        scratch_shapes=[
            pltpu.VMEM((seq // 2, HEAD_DIM), bf16),
            pltpu.VMEM((seq, HEAD_DIM), bf16),
            pltpu.VMEM((seq, HEAD_DIM), bf16),
            pltpu.VMEM((n, 1, rows), jnp.int32),
            pltpu.VMEM((seq, 2 * width), bf16),
            pltpu.VMEM((2 * wrows, wcols // 2), bf16),
            pltpu.VMEM((seq, wcols // 2), bf16),
            pltpu.VMEM((8, rows, wcols // 2), bf16),
            pltpu.VMEM(residual.shape, bf16),
            dma((n,)), dma((n // 2,)),
            dma((n,)), dma((n,)),
            dma((n,)), dma((n,)),
            dma((n,)), dma((n,)),
            dma((n,)), dma((n,)),
            dma((n,)), dma((n,)),
            dma((n,)), dma((8,)),
            dma((3,)), dma,
        ],
        compiler_params=pltpu.CompilerParams(collective_id=0, has_side_effects=True),
    )(query, key_states, value_states, doc_ids.reshape(1, rows), out_weight, residual)


def solution(mesh):
    placed = (
        P("seq", "head"),
        P("seq", "head"),
        P("seq", "head"),
        P("seq"),
        P("head", "seq"),
        P("seq", "head"),
    )
    n, nh = mesh.shape["seq"], mesh.shape["head"]

    def body(query, key_states, value_states, doc_ids, out_weight, residual):
        heads = query.shape[1] // HEAD_DIM
        fits = (
            n == 2 * heads
            and n == 2 * nh
            and nh % 2 == 0
            and out_weight.shape[1] % 256 == 0
            and query.shape[0] % 16 == 0
        )
        run = functools.partial(fused, n, nh) if fits else shards
        return run(query, key_states, value_states, doc_ids, out_weight, residual)

    return jax.shard_map(
        body, mesh=mesh, in_specs=placed, out_specs=P("seq", "head"), check_vma=False
    )
```

```python
import functools

import jax
import jax.numpy as jnp
from jax import lax
from jax.experimental import pallas as pl
from jax.experimental.pallas import tpu as pltpu
from jax.sharding import PartitionSpec as P

HEAD_DIM = 128


masked_score = -1e30


def to_heads(block):
    return block.reshape(block.shape[0], block.shape[1] // HEAD_DIM, HEAD_DIM)


def attend_block(state, queries, query_pos, query_docs, keys, values, key_pos, key_docs):
    run_max, run_sum, run_acc = state
    scores = jnp.einsum(
        "qhd,khd->hqk", queries, keys, preferred_element_type=jnp.float32
    ) * HEAD_DIM ** (-0.5)
    allowed = (key_pos[None, :] <= query_pos[:, None]) & (key_docs[None, :] == query_docs[:, None])
    scores = jnp.where(allowed[None], scores, masked_score)
    new_max = jnp.maximum(run_max, jnp.max(scores, axis=-1))
    weights = jnp.where(allowed[None], jnp.exp(scores - new_max[..., None]), 0.0)
    run_sum = jnp.sum(weights, axis=-1)
    run_acc = jnp.einsum(
        "hqk,khd->hqd", weights.astype(jnp.bfloat16), values, preferred_element_type=jnp.float32
    )
    return (new_max, run_sum, run_acc)


def shards(query, key_states, value_states, doc_ids, out_weight, residual):
    tok_rows = query.shape[0]
    heads = query.shape[1] // HEAD_DIM
    shard_index = lax.axis_index("seq")
    first_pos = shard_index * tok_rows
    groups = [(query, first_pos + jnp.arange(tok_rows, dtype=jnp.int32), doc_ids)]
    prepared = [(to_heads(block), block_pos, block_docs) for block, block_pos, block_docs in groups]
    initial = tuple(
        (
            (
                jnp.full((heads, block_pos.shape[0]), masked_score, jnp.float32),
                jnp.zeros((heads, block_pos.shape[0]), jnp.float32),
                jnp.zeros((heads, block_pos.shape[0], HEAD_DIM), jnp.float32),
            )
            for block, block_pos, block_docs in groups
        )
    )
    first_row = jnp.int32(0)
    keys = lax.all_gather(key_states, "seq", axis=0, tiled=True)
    values = lax.all_gather(value_states, "seq", axis=0, tiled=True)
    key_docs = lax.all_gather(doc_ids, "seq", axis=0, tiled=True)
    key_pos = jnp.arange(keys.shape[0], dtype=jnp.int32)
    key_heads = to_heads(keys)
    value_heads = to_heads(values)
    updated = []
    for member, state in zip(prepared, initial):
        queries, query_pos, query_docs = member

        def advance(inner, queries=queries, query_pos=query_pos, query_docs=query_docs):
            return attend_block(
                inner, queries, query_pos, query_docs, key_heads, value_heads, key_pos, key_docs
            )

        def unchanged(inner):
            return inner

        updated.append(lax.cond(first_row <= jnp.max(query_pos), advance, unchanged, state))
    finals = tuple(updated)
    outputs = []
    for run_max, run_sum, run_acc in finals:
        normed = run_acc / run_sum[..., None]
        outputs.append(
            jnp.transpose(normed, (1, 0, 2))
            .reshape(normed.shape[1], heads * HEAD_DIM)
            .astype(jnp.bfloat16)
        )
    attended = outputs[0]
    mapped = jnp.dot(
        attended,
        lax.all_gather(out_weight, "seq", axis=1, tiled=True),
        preferred_element_type=jnp.float32,
    )
    summed = lax.psum_scatter(mapped, "head", scatter_dimension=1, tiled=True)
    return (residual.astype(jnp.float32) + summed).astype(jnp.bfloat16)


MESH = pl.DeviceIdType.MESH


CHUNKS = 2


def attention(queries, keys, values, doc_row, first_row, pos_rows):
    rows, keep = queries.shape[0], keys.shape[0]
    scores = lax.dot_general(
        queries, keys, (((1,), (1,)), ((), ())), preferred_element_type=jnp.float32
    ) * HEAD_DIM ** (-0.5)
    row_pos = lax.broadcasted_iota(jnp.int32, (rows, keep), 0) + first_row
    col_pos = lax.broadcasted_iota(jnp.int32, (rows, keep), 1)
    docs = jnp.broadcast_to(doc_row, (rows, keep))
    query_docs = jnp.sum(jnp.where(row_pos == col_pos, docs, 0), axis=1, keepdims=True)
    allowed = (col_pos <= row_pos) & (docs == query_docs)
    scores = jnp.where(allowed, scores, masked_score)
    row_max = jnp.max(scores, axis=1, keepdims=True)
    weights = jnp.where(allowed, jnp.exp(scores - row_max), 0.0)
    row_sum = jnp.sum(weights, axis=1, keepdims=True)
    product = jnp.dot(weights.astype(jnp.bfloat16), values, preferred_element_type=jnp.float32)
    return (product / row_sum).astype(jnp.bfloat16)


def fused_kernel(
    n, nh, q_ref, k_ref, v_ref, doc_ref, w_ref, res_ref, out_ref,
    qbuf, kbuf, vbuf, docbuf, att, wbuf, sendbuf, parts, resbuf,
    q_send, q_recv, k_send, k_recv, v_send, v_recv, d_send, d_recv,
    z_send, z_recv, f_send, f_recv, p_send, p_recv, w_sems, w_recv, res_sem,
):
    me = lax.axis_index("seq")
    head = lax.axis_index("head")
    rows = k_ref.shape[0]
    half = n // 2
    mid = half * rows
    plane, side = me // 2, me % 2
    my_half = me // half
    pair, core = head // 2, head % 2
    partner = pair * 2 + (1 - core)
    wrows, wcols = w_ref.shape
    w_slot = wbuf.at[pl.ds(pl.multiple_of(core * wrows, wrows), wrows), :]

    res_copy = pltpu.make_async_copy(res_ref, resbuf, res_sem)
    res_copy.start()

    barrier = pltpu.get_barrier_semaphore()
    for ds_ in range(n):
        for dh in range(nh):
            if ds_ == 0 and dh == 0:
                continue
            pl.semaphore_signal(
                barrier, inc=1,
                device_id=(lax.rem(me + ds_, n), lax.rem(head + dh, nh)),
                device_id_type=MESH,
            )
    pl.semaphore_wait(barrier, n * nh - 1)

    def block(ref, source):
        return ref.at[pl.ds(pl.multiple_of(source * rows, rows), rows), :]

    def lanes(ref, index):
        return ref.at[:, pl.ds(pl.multiple_of(index * HEAD_DIM, HEAD_DIM), HEAD_DIM)]

    def send_kv(kind, dst):
        src, dest, ssem, rsem = kind
        return pltpu.make_async_remote_copy(
            src_ref=lanes(src, dst // 2), dst_ref=block(dest, me),
            send_sem=ssem.at[dst], recv_sem=rsem.at[me],
            device_id=(dst, head), device_id_type=MESH,
        )

    def local_kv(kind):
        src, dest, ssem, rsem = kind
        return pltpu.make_async_copy(lanes(src, plane), block(dest, me), rsem.at[me])

    def send_q(dst):
        return pltpu.make_async_remote_copy(
            src_ref=lanes(q_ref, dst // 2), dst_ref=block(qbuf, me % half),
            send_sem=q_send.at[dst], recv_sem=q_recv.at[me % half],
            device_id=(dst, head), device_id_type=MESH,
        )

    def send_doc(dst):
        return pltpu.make_async_remote_copy(
            src_ref=doc_ref, dst_ref=docbuf.at[me],
            send_sem=d_send.at[dst], recv_sem=d_recv.at[me],
            device_id=(dst, head), device_id_type=MESH,
        )

    kinds = ((k_ref, kbuf, k_send, k_recv), (v_ref, vbuf, v_send, v_recv))

    for off in range(1, n):
        dst = lax.rem(me + off, n)

        @pl.when((dst % 2 == 1) | (my_half == 0))
        def _(dst=dst):
            send_kv(kinds[0], dst).start()

        @pl.when(dst % 2 == my_half)
        def _(dst=dst):
            send_q(dst).start()

        send_doc(dst).start()

        @pl.when((dst % 2 == 1) | (my_half == 0))
        def _(dst=dst):
            send_kv(kinds[1], dst).start()

    def w_send(to, sem):
        return pltpu.make_async_remote_copy(
            src_ref=w_ref, dst_ref=w_slot, send_sem=w_sems.at[sem], recv_sem=w_recv.at[core],
            device_id=to, device_id_type=MESH,
        )

    w_across = w_send((2 * plane + 1 - side, pair * 2 + side), 0)
    w_beside = w_send((me, partner), 1)
    w_across.start()

    @pl.when(core == side)
    def _():
        pltpu.make_async_copy(w_ref, w_slot, w_recv.at[core]).start()

    @pl.when(core != side)
    def _():
        w_beside.start()

    @pl.when((side == 1) | (my_half == 0))
    def _():
        for kind in kinds:
            local_kv(kind).start()

    @pl.when(side == my_half)
    def _():
        pltpu.make_async_copy(
            lanes(q_ref, plane), block(qbuf, me % half), q_recv.at[me % half]
        ).start()

    pltpu.make_async_copy(doc_ref, docbuf.at[me], d_recv.at[me]).start()

    def arrived(ref, sem):
        pltpu.make_async_copy(ref, ref, sem).wait()

    for source in range(n):
        arrived(docbuf.at[source], d_recv.at[source])
    for source in range(half):
        arrived(qbuf.at[pl.ds(source * rows, rows), :], q_recv.at[source])
        for _, dest, _, rsem in kinds:
            arrived(dest.at[pl.ds(source * rows, rows), :], rsem.at[source])

    doc_row = jnp.concatenate([docbuf[source] for source in range(n)], axis=1)

    @pl.when(side == 0)
    def _():
        att[core * half + plane] = attention(
            qbuf[...], kbuf[:mid, :], vbuf[:mid, :], doc_row[:, :mid], 0, mid
        )

    @pl.when(side == 1)
    def _():
        for source in range(half, n):
            for _, dest, _, rsem in kinds:
                arrived(dest.at[pl.ds(source * rows, rows), :], rsem.at[source])
        att[core * half + plane] = attention(
            qbuf[...], kbuf[...], vbuf[...], doc_row, mid, mid
        )

    chunk = mid // CHUNKS

    def att_chunk(c, source, part):
        start = part * chunk
        return att.at[
            c * half + source // 2, pl.ds(pl.multiple_of(start, chunk), chunk), :
        ]

    def att_copy(source, part, send, recv, to):
        ref = att_chunk(core, source, part)
        return pltpu.make_async_remote_copy(
            src_ref=ref, dst_ref=ref, send_sem=send, recv_sem=recv,
            device_id=to, device_id_type=MESH,
        )

    def along(dz, part):
        return att_copy(
            me, part, z_send.at[dz, part], z_recv.at[plane, part], (2 * dz + side, head)
        )

    def forward(source, part):
        return att_copy(
            source, part, f_send.at[source // 2, part], f_recv.at[source // 2, part], (me, partner)
        )

    offsets = list(range(1, half))
    near_first = sorted(offsets, key=lambda off: min(off, half - off))
    for off in reversed(near_first):
        for part in range(CHUNKS):
            along(lax.rem(plane + off, half), part).start()
    for part in range(CHUNKS):
        forward(me, part).start()

    for off in near_first:
        sz = lax.rem(plane + off, half)
        for part in range(CHUNKS):
            arrived(att_chunk(core, 2 * sz + side, part), z_recv.at[sz, part])
            forward(2 * sz + side, part).start()

    for slot in range(2):
        arrived(wbuf.at[pl.ds(slot * wrows, wrows), :], w_recv.at[slot])
    for sz in range(half):
        for part in range(CHUNKS):
            arrived(att_chunk(1 - core, 2 * sz + side, part), f_recv.at[sz, part])
    attended = jnp.concatenate([att[index] for index in range(n)], axis=1)
    sendbuf[...] = jnp.dot(
        attended, wbuf[...], preferred_element_type=jnp.float32
    ).astype(jnp.bfloat16)
    slot = pair * 2 + core
    for index in range(half):
        target = side * half + index
        src = sendbuf.at[pl.ds(index * rows, rows), :]
        own = (me == target) & (head == plane)

        @pl.when(own)
        def _(src=src):
            pltpu.make_async_copy(src, parts.at[slot], p_recv.at[slot]).start()

        @pl.when(jnp.logical_not(own))
        def _(src=src, target=target, index=index):
            pltpu.make_async_remote_copy(
                src_ref=src, dst_ref=parts.at[slot],
                send_sem=p_send.at[index], recv_sem=p_recv.at[slot],
                device_id=(target, plane), device_id_type=MESH,
            ).start()

    res_copy.wait()
    for c in range(2):
        for p in range(2):
            arrived(parts.at[2 * p + c], p_recv.at[2 * p + c])
        cols = slice(c * wcols, (c + 1) * wcols)
        total = parts[c].astype(jnp.float32) + parts[2 + c].astype(jnp.float32)
        out_ref[:, cols] = (resbuf[:, cols].astype(jnp.float32) + total).astype(jnp.bfloat16)

    for off in range(1, n):
        dst = lax.rem(me + off, n)

        @pl.when((dst % 2 == 1) | (my_half == 0))
        def _(dst=dst):
            for kind in kinds:
                send_kv(kind, dst).wait_send()

        @pl.when(dst % 2 == my_half)
        def _(dst=dst):
            send_q(dst).wait_send()

        send_doc(dst).wait_send()
    for part in range(CHUNKS):
        for off in near_first:
            along(lax.rem(plane + off, half), part).wait_send()
        for sz in range(half):
            forward(2 * sz + side, part).wait_send()
    w_across.wait_send()

    @pl.when(core != side)
    def _():
        w_beside.wait_send()

    for index in range(half):
        src = sendbuf.at[pl.ds(index * rows, rows), :]

        @pl.when(jnp.logical_not((me == side * half + index) & (head == plane)))
        def _(src=src, index=index):
            pltpu.make_async_copy(src, src, p_send.at[index]).wait()


def fused(n, nh, query, key_states, value_states, doc_ids, out_weight, residual):
    rows, width = key_states.shape
    wrows, wcols = out_weight.shape
    seq = n * rows
    dma = pltpu.SemaphoreType.DMA
    vmem = pl.BlockSpec(memory_space=pltpu.VMEM)
    any_ = pl.BlockSpec(memory_space=pl.ANY)
    bf16 = jnp.bfloat16
    return pl.pallas_call(
        functools.partial(fused_kernel, n, nh),
        out_shape=jax.ShapeDtypeStruct(residual.shape, residual.dtype),
        in_specs=[vmem, vmem, vmem, vmem, any_, any_],
        out_specs=vmem,
        scratch_shapes=[
            pltpu.VMEM((seq // 2, HEAD_DIM), bf16),
            pltpu.VMEM((seq, HEAD_DIM), bf16),
            pltpu.VMEM((seq, HEAD_DIM), bf16),
            pltpu.VMEM((n, 1, rows), jnp.int32),
            pltpu.VMEM((n, seq // 2, HEAD_DIM), bf16),
            pltpu.VMEM((2 * wrows, wcols), bf16),
            pltpu.VMEM((seq // 2, wcols), bf16),
            pltpu.VMEM((4, rows, wcols), bf16),
            pltpu.VMEM(residual.shape, bf16),
            dma((n,)), dma((n // 2,)),
            dma((n,)), dma((n,)),
            dma((n,)), dma((n,)),
            dma((n,)), dma((n,)),
            dma((n // 2, CHUNKS)), dma((n // 2, CHUNKS)),
            dma((n // 2, CHUNKS)), dma((n // 2, CHUNKS)),
            dma((n // 2,)), dma((4,)),
            dma((2,)), dma((2,)), dma,
        ],
        compiler_params=pltpu.CompilerParams(collective_id=0, has_side_effects=True),
    )(query, key_states, value_states, doc_ids.reshape(1, rows), out_weight, residual)


def solution(mesh):
    placed = (
        P("seq", "head"),
        P("seq", "head"),
        P("seq", "head"),
        P("seq"),
        P("head", "seq"),
        P("seq", "head"),
    )
    n, nh = mesh.shape["seq"], mesh.shape["head"]

    def body(query, key_states, value_states, doc_ids, out_weight, residual):
        heads = query.shape[1] // HEAD_DIM
        fits = (
            n == 2 * heads
            and n == 2 * nh
            and nh % 2 == 0
            and out_weight.shape[1] % 256 == 0
            and query.shape[0] % 16 == 0
        )
        run = functools.partial(fused, n, nh) if fits else shards
        return run(query, key_states, value_states, doc_ids, out_weight, residual)

    return jax.shard_map(
        body, mesh=mesh, in_specs=placed, out_specs=P("seq", "head"), check_vma=False
    )
```
